32 devices in a mesh: group: 4 (over y, core), member: 8 (over z, x).
Axes of the slice: x: 2, y: 2, z: 4, core: 2. Of those that a mesh axis runs over, the one named last changes fastest.
Arguments:
- off_tiles: bfloat16 [64, 8, 128, 128], P(('group', 'member')), may hold values from -0.1875 to 0.1875
- off_cols: int32 [64, 8], P(('group', 'member')), may hold values from 0 to 17
- member_send: int32 [32, 8, 1], P(('group', 'member')), may hold values from 0 to 1
- group_send: int32 [32, 4], P(('group', 'member')), may hold values from 0 to 1
- diag_tiles: bfloat16 [64, 128, 128], P(('group', 'member')), may hold values from -1 to 9
- smoother: bfloat16 [64, 128, 128], P(('group', 'member')), may hold values from -1 to 1
- agg_map: int32 [64], P(('group', 'member')), may hold values from 0 to 1
- prolong: bfloat16 [64, 128, 128], P(('group', 'member')), may hold values from -0.5 to 0.5
- coarse_inv: bfloat16 [1024, 1024], P(None, 'group'), may hold values from -0.03125 to 0.03125
- krylov_basis: bfloat16 [64, 32, 128], P(('group', 'member')), may hold values from -24 to 24, as said below
Outputs:
- preconditioned: bfloat16 [64, 8, 128], P(('group', 'member'))
- coefficients: float32 [32, 8], replicated
- gram_matrix: float32 [8, 8], replicated
- new_block: float32 [64, 8, 128], P(('group', 'member'))
The draws below stay inside these ranges and needn't reach their ends.
Inputs may be any that keep to these rules, and one draw needn't show every extreme that they name: `off_cols`: entries below 2 name the device's own row tiles; entry 2 + p + s names slot s of what member p of the same group sends; the last 8 entries name what the groups below and above send. `member_send`: entry [d, p, s] is the local row tile that device d sends to member p of its group in slot s. `group_send`: entry [d, s] is the local row tile that device d sends, in slot s, to the same member of the groups below and above. `krylov_basis`: the 32 basis vectors are orthonormal, up to bfloat16 rounding, under the inner product (1 / 8192) times the sum over all rows.
All inputs are finite; a program needn't handle non-finite values.
Results may differ from the reference program's by a relative error of at most 0.02.
Values may be sent and summed in bfloat16 or wider, within the bound.
No kernel may reach another device: no remote copies, remote signals or barrier semaphores. Data moves between devices by JAX's collectives and lax.ppermute only.
A program may use at most 64 MiB of HBM per device.

```python
import math
import jax
import jax.numpy as jnp
from jax import lax

TILE = 128
NVEC = 8
K = 8
GH = 1
GG = 4
CTG = 2
TD = 2
NT = 64
ROWS = 8192
NB = 32
NCT = 8
NC = 1024
N_GROUP = 4
N_MEMBER = 8


def pivot_values(key):
    logs = jax.random.uniform(jax.random.fold_in(key, 11), (NT, TILE), jnp.float32, math.log(2.0), math.log(6.0))
    return jnp.exp(logs)


def draw_diag_tiles(key, part):
    pivots = pivot_values(key)
    noise = jnp.clip(jax.random.normal(jax.random.fold_in(key, 12), (NT, TILE, TILE), jnp.float32), -6.0, 6.0)
    noise = noise * (0.8 / math.sqrt(TILE))
    identity = jnp.eye(TILE, dtype=jnp.float32)
    return (noise + identity[None, :, :] * pivots[:, :, None]).astype(jnp.bfloat16)


def draw_smoother(key, part):
    pivots = pivot_values(key)
    noise = jnp.clip(jax.random.normal(jax.random.fold_in(key, 13), (NT, TILE, TILE), jnp.float32), -6.0, 6.0)
    noise = noise * (0.1 / math.sqrt(TILE))
    identity = jnp.eye(TILE, dtype=jnp.float32)
    return (0.7 * (noise + identity[None, :, :] / pivots[:, :, None])).astype(jnp.bfloat16)


def draw_krylov_basis(key, part):
    position = jnp.arange(NT, dtype=jnp.float32) / (NT - 1)
    rough = jnp.exp(jax.random.uniform(jax.random.fold_in(key, 21), (NT, NB, 1), jnp.float32, 0.0, math.log(2.0)))
    ramp = 1.0 + 2.0 * position
    base = jnp.clip(jax.random.normal(jax.random.fold_in(key, 22), (NT, NB, TILE), jnp.float32), -4.0, 4.0)
    values = base * ramp[:, None, None] * rough
    matrix = jnp.transpose(values, (0, 2, 1)).reshape(NT * TILE, NB)
    ortho, upper = jnp.linalg.qr(matrix)
    ortho = ortho * math.sqrt(NT * TILE)
    values = jnp.transpose(ortho.reshape(NT, TILE, NB), (0, 2, 1))
    return jnp.clip(values, -24.0, 24.0).astype(jnp.bfloat16)


def place_ends(values, key, smallest, top_value):
    longest = values.shape.index(max(values.shape))
    spots = []
    for shift in (0, 1):
        where = [jax.random.randint(jax.random.fold_in(key, axis), (), 0, length) for axis, length in enumerate(values.shape)]
        where[longest] = (where[longest] + shift) % values.shape[longest]
        spots.append(tuple(where))
    return values.at[spots[0]].set(smallest).at[spots[1]].set(top_value)


def block_scale(own_key, shape, cuts, low, largest):
    gain = 1.0
    for axis_at, parts in cuts:
        heights = jax.random.uniform(jax.random.fold_in(jax.random.fold_in(own_key, 6), axis_at), (parts,), jnp.float32, low / len(cuts), largest / len(cuts))
        gain = gain * jnp.repeat(jnp.exp(heights), shape[axis_at] // parts).reshape((-1,) + (1,) * (len(shape) - 1 - axis_at))
    return gain


def centred(rng, dims, width, reach, split=(), kind=jnp.bfloat16):
    array = width * jax.random.normal(rng, dims, jnp.float32)
    if split:
        array = array * block_scale(rng, dims, split, -0.22, 0.18)
    return jnp.clip(array, -reach, reach).astype(kind)


def setup_inputs(seed: int = 0) -> dict:
    seeds = jax.random.split(jax.random.key(seed), 11)
    return {
        "off_tiles": centred(seeds[0], (NT, K, TILE, TILE), (K * TILE) ** -0.5, 0.1875, ((0, 32),)),
        "off_cols": place_ends(jax.random.randint(seeds[1], (NT, K), 0, TD + N_MEMBER * GH + 2 * GG), jax.random.fold_in(seeds[1], 1), 0, (TD + N_MEMBER * GH + 2 * GG) - 1).astype(jnp.int32),
        "member_send": place_ends(jax.random.randint(seeds[2], (N_GROUP * N_MEMBER, N_MEMBER, GH), 0, TD), jax.random.fold_in(seeds[2], 1), 0, TD - 1).astype(jnp.int32),
        "group_send": place_ends(jax.random.randint(seeds[3], (N_GROUP * N_MEMBER, GG), 0, TD), jax.random.fold_in(seeds[3], 1), 0, TD - 1).astype(jnp.int32),
        "diag_tiles": draw_diag_tiles(jax.random.fold_in(seeds[10], 71), 0),
        "smoother": draw_smoother(jax.random.fold_in(seeds[10], 71), 0),
        "agg_map": place_ends(jax.random.randint(seeds[6], (NT,), 0, CTG), jax.random.fold_in(seeds[6], 1), 0, CTG - 1).astype(jnp.int32),
        "prolong": centred(seeds[7], (NT, TILE, TILE), TILE ** -0.5, 0.5, ((0, 32),)),
        "coarse_inv": centred(seeds[8], (NC, NC), (4 * NC * TD * N_MEMBER // CTG) ** -0.5, 0.03125, ((1, 4),)),
        "krylov_basis": draw_krylov_basis(jax.random.fold_in(seeds[10], 71), 0),
    }


def ghost_sources(member_send, group_send):
    devices = N_GROUP * N_MEMBER
    device_ids = jnp.arange(devices, dtype=jnp.int32)
    group_ids = device_ids // N_MEMBER
    member_ids = device_ids % N_MEMBER
    own_tiles = device_ids[:, None] * TD + jnp.arange(TD, dtype=jnp.int32)[None, :]
    peer_ids = group_ids[:, None] * N_MEMBER + jnp.arange(N_MEMBER, dtype=jnp.int32)[None, :]
    slot_ids = member_send[peer_ids, member_ids[:, None], :]
    remote = (peer_ids[:, :, None] * TD + slot_ids).reshape(devices, N_MEMBER * GH)
    below = jnp.maximum(device_ids - N_MEMBER, 0)
    above = jnp.minimum(device_ids + N_MEMBER, devices - 1)
    lower_tiles = jnp.where(group_ids[:, None] > 0, below[:, None] * TD + group_send[below], NT)
    upper_tiles = jnp.where(group_ids[:, None] < N_GROUP - 1, above[:, None] * TD + group_send[above], NT)
    return jnp.concatenate([own_tiles, remote, lower_tiles, upper_tiles], axis=1).astype(jnp.int32)

def operate(values, off_tiles, global_cols, diag_tiles):
    padded = jnp.concatenate([values, jnp.zeros((1, NVEC, TILE), values.dtype)], axis=0)

    def per_device(device):
        offset = (device * TD).astype(jnp.int32)
        columns = lax.dynamic_slice_in_dim(global_cols, offset, TD, 0)
        tiles = lax.dynamic_slice_in_dim(off_tiles, offset, TD, 0).astype(jnp.float32)
        picked = padded[columns].astype(jnp.float32)
        own_part = lax.dynamic_slice_in_dim(values, offset, TD, 0).astype(jnp.float32)
        diagonal = lax.dynamic_slice_in_dim(diag_tiles, offset, TD, 0).astype(jnp.float32)
        far_part = jnp.einsum('tkcj,tkji->tci', picked, tiles, precision=lax.Precision.HIGHEST)
        near_part = jnp.einsum('tcj,tji->tci', own_part, diagonal, precision=lax.Precision.HIGHEST)
        return near_part + far_part
    result = lax.map(per_device, jnp.arange(N_GROUP * N_MEMBER, dtype=jnp.int32))
    return result.reshape(NT, NVEC, TILE)

def tilewise(left_side, tiles):
    return jnp.einsum('tcj,tji->tci', left_side.astype(jnp.float32), tiles.astype(jnp.float32), precision=lax.Precision.HIGHEST)

def reference(off_tiles, off_cols, member_send, group_send, diag_tiles, smoother, agg_map, prolong, coarse_inv, krylov_basis):
    sources = ghost_sources(member_send, group_send)
    owners = jnp.arange(NT, dtype=jnp.int32) // TD
    global_cols = sources[owners[:, None], off_cols].astype(jnp.int32)
    last_block = krylov_basis[:, NB - NVEC:, :]
    block_wide = last_block.astype(jnp.float32)
    first = tilewise(last_block, smoother).astype(jnp.bfloat16)
    residual_one = (block_wide - operate(first, off_tiles, global_cols, diag_tiles)).astype(jnp.bfloat16)
    pieces = jnp.einsum('tci,tji->tcj', residual_one.astype(jnp.float32), prolong.astype(jnp.float32), precision=lax.Precision.HIGHEST)
    coarse_ids = (jnp.arange(NT, dtype=jnp.int32) // (TD * N_MEMBER) * CTG + agg_map).astype(jnp.int32)
    coarse_rhs = jax.ops.segment_sum(pieces, coarse_ids, num_segments=NCT)
    coarse_round = coarse_rhs.astype(jnp.bfloat16)
    columns = coarse_inv.astype(jnp.float32).reshape(NCT, TILE, NC)
    correction = jnp.einsum('acj,ajo->co', coarse_round.astype(jnp.float32), columns, precision=lax.Precision.HIGHEST)
    correction = correction.astype(jnp.bfloat16).reshape(NVEC, NCT, TILE)
    chosen = jnp.transpose(correction[:, coarse_ids, :], (1, 0, 2))
    second = (first.astype(jnp.float32) + tilewise(chosen, prolong)).astype(jnp.bfloat16)
    residual_two = (block_wide - operate(second, off_tiles, global_cols, diag_tiles)).astype(jnp.bfloat16)
    preconditioned = (second.astype(jnp.float32) + tilewise(residual_two, smoother)).astype(jnp.bfloat16)
    applied = operate(preconditioned, off_tiles, global_cols, diag_tiles).astype(jnp.bfloat16)
    basis_wide = krylov_basis.astype(jnp.float32)
    coefficients = jnp.einsum('tpi,tci->pc', basis_wide, applied.astype(jnp.float32), precision=lax.Precision.HIGHEST) * (1.0 / ROWS)
    remainder = applied.astype(jnp.float32) - jnp.einsum('pc,tpi->tci', coefficients, basis_wide, precision=lax.Precision.HIGHEST)
    gram_matrix = jnp.einsum('tci,tdi->cd', remainder, remainder, precision=lax.Precision.HIGHEST) * (1.0 / ROWS)
    factor = jnp.linalg.cholesky(gram_matrix)
    inverse = lax.linalg.triangular_solve(factor, jnp.eye(NVEC, dtype=jnp.float32), left_side=True, lower=True)
    new_block = jnp.einsum('cd,tdi->tci', inverse, remainder, precision=lax.Precision.HIGHEST)
    return (preconditioned, coefficients, gram_matrix, new_block)
```

```python
import functools

import jax
import jax.numpy as jnp
from jax import lax
from jax.experimental import pallas as pl
from jax.experimental.pallas import tpu as pltpu
from jax.sharding import PartitionSpec as P

AXES = ("group", "member")
F32 = jnp.float32
BF16 = jnp.bfloat16
HIGH = lax.Precision.HIGHEST


def dot(left, right, contract=(1, 0), precision=None):
    return lax.dot_general(
        left,
        right,
        (((contract[0],), (contract[1],)), ((), ())),
        precision=precision,
        preferred_element_type=F32,
    )


def place():
    group, member = lax.axis_index("group"), lax.axis_index("member")
    return group, member, lax.axis_size("group"), lax.axis_size("member")


def fill_halo(send_ref, tiles_ref, member_send_ref):
    group, _, _, members = place()
    slots = member_send_ref.shape[2]
    count = tiles_ref.shape[0]
    everything = tiles_ref[...]
    send_ref[:, :count] = jnp.broadcast_to(everything[None], (send_ref.shape[0], *everything.shape))

    def one(peer, carry):
        for slot in range(slots):
            send_ref[group * members + peer, slot] = tiles_ref[member_send_ref[0, peer, slot]]
        return carry

    lax.fori_loop(0, members, one, 0, unroll=min(members, 8))


def fill_extended(ext_ref, own_ref, got_ref, table_ref, ghosts, rims):
    group, member, groups, members = place()
    count = own_ref.shape[0]
    ext_ref[:count] = own_ref[...]

    def one(peer, carry):
        for slot in range(ghosts):
            ext_ref[count + peer * ghosts + slot] = got_ref[group * members + peer, slot]
        return carry

    lax.fori_loop(0, members, one, 0, unroll=min(members, 8))
    base = count + members * ghosts
    for side in range(2):
        other = group - 1 if side == 0 else group + 1
        other = jnp.clip(other, 0, groups - 1)
        source = other * members + member
        tiles = [got_ref[source, j].astype(F32) for j in range(count)]
        for slot in range(rims):
            which = jnp.broadcast_to(table_ref[side, slot : slot + 1, :], tiles[0].shape)
            value = jnp.zeros_like(tiles[0])
            for j in range(count):
                value = jnp.where(which == j, tiles[j], value)
            ext_ref[base + side * rims + slot] = value.astype(BF16)


def apply_row(tile, ext_ref, own_ref, off_ref, cols_ref, diag_ref):
    total = dot(own_ref[tile], diag_ref[tile])
    for k in range(off_ref.shape[1]):
        total = total + dot(ext_ref[cols_ref[tile, k]], off_ref[tile, k])
    return total


def kernel_start(basis_ref, smoother_ref, member_send_ref, group_send_ref, first_ref, send_ref):
    count, vectors, width = first_ref.shape
    before = basis_ref.shape[1] - vectors
    for tile in range(count):
        first_ref[tile] = dot(basis_ref[tile, before:, :], smoother_ref[tile]).astype(BF16)
    fill_halo(send_ref, first_ref, member_send_ref)
    rows = lax.broadcasted_iota(jnp.int32, (vectors, width), 0)
    table = jnp.zeros((vectors, width), F32)
    for slot in range(group_send_ref.shape[1]):
        table = jnp.where(rows == slot, group_send_ref[0, slot].astype(F32), table)
    send_ref[:, count] = jnp.broadcast_to(table.astype(BF16)[None], (send_ref.shape[0], vectors, width))


def kernel_restrict(
    ghosts, rims, first_ref, got_ref, basis_ref, off_ref, cols_ref, diag_ref, prolong_ref, agg_ref,
    send_ref, table_ref, ext_ref,
):
    group, member, groups, members = place()
    count, vectors, _ = first_ref.shape
    before = basis_ref.shape[1] - vectors
    coarse = send_ref.shape[1]
    for side in range(2):
        other = group - 1 if side == 0 else group + 1
        inside = jnp.logical_and(other >= 0, other < groups)
        source = jnp.clip(other, 0, groups - 1) * members + member
        table = got_ref[source, count].astype(F32)
        table_ref[side] = jnp.where(inside, table, -1.0)
    fill_extended(ext_ref, first_ref, got_ref, table_ref, ghosts, rims)
    parts = [None] * coarse
    for tile in range(count):
        right = basis_ref[tile, before:, :].astype(F32)
        residual = (right - apply_row(tile, ext_ref, first_ref, off_ref, cols_ref, diag_ref)).astype(BF16)
        piece = dot(residual, prolong_ref[tile], (1, 1))
        for a in range(coarse):
            term = jnp.where(agg_ref[tile] == a, piece, 0.0)
            parts[a] = term if parts[a] is None else parts[a] + term
    for a in range(coarse):
        send_ref[:, a] = jnp.broadcast_to(parts[a].astype(BF16)[None], (send_ref.shape[0], *parts[a].shape))


def kernel_coarse(
    got_ref, inverse_ref, first_ref, prolong_ref, agg_ref, member_send_ref, second_ref, send_ref, fix_ref
):
    _, _, groups, members = place()
    count, vectors, width = first_ref.shape
    coarse = got_ref.shape[1]
    total = None
    for g in range(groups):
        for a in range(coarse):
            part = got_ref[g * members, a].astype(F32)
            for m in range(1, members):
                part = part + got_ref[g * members + m, a].astype(F32)
            start = (g * coarse + a) * width
            term = dot(part.astype(BF16), inverse_ref[start : start + width, :])
            total = term if total is None else total + term
    for a in range(coarse):
        fix_ref[a] = total[:, a * width : (a + 1) * width].astype(BF16)
    for tile in range(count):
        step = dot(fix_ref[agg_ref[tile]], prolong_ref[tile])
        second_ref[tile] = (first_ref[tile].astype(F32) + step).astype(BF16)
    fill_halo(send_ref, second_ref, member_send_ref)


def kernel_smooth(
    ghosts, rims, second_ref, got_ref, table_ref, basis_ref, off_ref, cols_ref, diag_ref, smoother_ref,
    member_send_ref, result_ref, send_ref, ext_ref,
):
    count, vectors, _ = second_ref.shape
    before = basis_ref.shape[1] - vectors
    fill_extended(ext_ref, second_ref, got_ref, table_ref, ghosts, rims)
    for tile in range(count):
        right = basis_ref[tile, before:, :].astype(F32)
        residual = (right - apply_row(tile, ext_ref, second_ref, off_ref, cols_ref, diag_ref)).astype(BF16)
        step = dot(residual, smoother_ref[tile])
        result_ref[tile] = (second_ref[tile].astype(F32) + step).astype(BF16)
    fill_halo(send_ref, result_ref, member_send_ref)


def pack_offsets(blocks):
    starts = []
    at = blocks + 1
    for i in range(blocks):
        starts.append(at)
        at += blocks - i
    return starts


def kernel_products(
    ghosts, rims, values_ref, got_ref, table_ref, basis_ref, off_ref, cols_ref, diag_ref,
    applied_ref, send_ref, ext_ref, wide_ref,
):
    count, vectors, width = values_ref.shape
    number = basis_ref.shape[1]
    blocks = number // vectors
    lanes = lax.broadcasted_iota(jnp.int32, (vectors, width), 1)
    fill_extended(ext_ref, values_ref, got_ref, table_ref, ghosts, rims)
    packed = None
    wide_ref[...] = jnp.zeros_like(wide_ref)
    for tile in range(count):
        applied = apply_row(tile, ext_ref, values_ref, off_ref, cols_ref, diag_ref).astype(BF16)
        applied_ref[tile] = applied
        wide_ref[:number] = basis_ref[tile].astype(F32)
        wide_ref[number : number + vectors] = applied.astype(F32)
        wide = wide_ref[...].astype(BF16)
        term = dot(applied, wide, (1, 1))
        for i, start in enumerate(pack_offsets(blocks)):
            own = dot(basis_ref[tile, i * vectors : (i + 1) * vectors, :], wide, (1, 1))
            moved = pltpu.roll(own, ((start - i) * vectors) % width, 1)
            inside = jnp.logical_and(lanes >= start * vectors, lanes < (start + blocks - i) * vectors)
            term = jnp.where(inside, moved, term)
        packed = term if packed is None else packed + term
    send_ref[...] = jnp.broadcast_to(packed[None], send_ref.shape)


def kernel_finish(scale, got_ref, applied_ref, basis_ref, coefficients_ref, gram_ref, block_ref, half_ref):
    count, vectors, width = applied_ref.shape
    number = basis_ref.shape[1]
    blocks = number // vectors
    total = jnp.sum(got_ref[...], axis=0) * scale
    turned = total[:, :number]
    own = total[:, number : number + vectors]
    coefficients_ref[...] = turned
    lanes = lax.broadcasted_iota(jnp.int32, (vectors, width), 1)
    rows = lax.broadcasted_iota(jnp.int32, (vectors, width), 0)
    for i, start in enumerate(pack_offsets(blocks)):
        moved = pltpu.roll(total, (i - start) * vectors % width, 1)
        first, last = i * vectors, (i + 1) * vectors
        inside = jnp.logical_and(lanes >= first, lanes < last)
        unit = jnp.where(lanes == rows + first, 1.0, 0.0)
        beyond = jnp.logical_and(lanes >= last, lanes < number)
        value = jnp.where(inside, unit - 0.5 * moved, jnp.where(beyond, -moved, 0.0))
        half_ref[i * vectors : (i + 1) * vectors, :] = value[:, :number]
    half = half_ref[...]
    weighted = dot(turned, half, (1, 1), HIGH)
    gram = own - dot(turned, weighted, (1, 1), HIGH) - dot(weighted, turned, (1, 1), HIGH)
    gram_ref[...] = gram
    square = lax.broadcasted_iota(jnp.int32, (vectors, vectors), 1)
    level = lax.broadcasted_iota(jnp.int32, (vectors, vectors), 0)
    left = gram
    right = jnp.where(square == level, 1.0, 0.0)
    for j in range(vectors):
        pivot = jnp.sqrt(left[j : j + 1, j : j + 1])
        line_left = left[j : j + 1, :] / pivot
        line_right = right[j : j + 1, :] / pivot
        factor = left[:, j : j + 1] / pivot
        below = level > j
        left = jnp.where(below, left - factor * line_left, left)
        right = jnp.where(below, right - factor * line_right, jnp.where(level == j, line_right, right))
    for tile in range(count):
        basis = basis_ref[tile].astype(F32)
        remainder = applied_ref[tile].astype(F32) - dot(turned, basis, (1, 0), HIGH)
        block_ref[tile] = dot(right, remainder, (1, 0), HIGH)


def spread(blocks):
    return lax.all_to_all(blocks, AXES, split_axis=0, concat_axis=0, tiled=True)


def local(
    off_tiles,
    off_cols,
    member_send,
    group_send,
    diag_tiles,
    smoother,
    agg_map,
    prolong,
    coarse_inv,
    krylov_basis,
):
    members = lax.axis_size("member")
    devices = lax.axis_size("group") * members
    count, width, _ = diag_tiles.shape
    number = krylov_basis.shape[1]
    ghosts, rims = member_send.shape[2], group_send.shape[1]
    coarse = coarse_inv.shape[1] // width
    extended = count + members * ghosts + 2 * rims
    vectors = 8
    tile = (vectors, width)
    halo = max(count, ghosts)
    vmem, smem = pl.BlockSpec(memory_space=pltpu.VMEM), pl.BlockSpec(memory_space=pltpu.SMEM)
    shape = jax.ShapeDtypeStruct
    ext = pltpu.VMEM((extended, *tile), BF16)

    def call(body, outs, ins, scratch=()):
        specs = [smem if a.dtype == jnp.int32 else vmem for a in ins]
        return pl.pallas_call(
            body,
            out_shape=tuple(outs),
            in_specs=specs,
            out_specs=tuple(vmem for _ in outs),
            scratch_shapes=scratch,
        )(*ins)

    own = shape((count, *tile), BF16)
    sent = shape((devices, halo, *tile), BF16)
    first, send = call(
        kernel_start,
        (own, shape((devices, halo + 1, *tile), BF16)),
        (krylov_basis, smoother, member_send, group_send),
    )
    send, table = call(
        functools.partial(kernel_restrict, ghosts, rims),
        (shape((devices, coarse, *tile), BF16), shape((2, *tile), F32)),
        (first, spread(send), krylov_basis, off_tiles, off_cols, diag_tiles, prolong, agg_map),
        (ext,),
    )
    second, send = call(
        kernel_coarse,
        (own, sent),
        (spread(send), coarse_inv, first, prolong, agg_map, member_send),
        (pltpu.VMEM((coarse, *tile), BF16),),
    )
    preconditioned, send = call(
        functools.partial(kernel_smooth, ghosts, rims),
        (own, sent),
        (second, spread(send), table, krylov_basis, off_tiles, off_cols, diag_tiles, smoother, member_send),
        (ext,),
    )
    applied, send = call(
        functools.partial(kernel_products, ghosts, rims),
        (own, shape((devices, *tile), F32)),
        (preconditioned, spread(send), table, krylov_basis, off_tiles, off_cols, diag_tiles),
        (ext, pltpu.VMEM((width, width), F32)),
    )
    turned, gram_matrix, new_block = call(
        functools.partial(kernel_finish, 1.0 / (count * width * devices)),
        (shape((vectors, number), F32), shape((vectors, vectors), F32), shape((count, *tile), F32)),
        (spread(send), applied, krylov_basis),
        (pltpu.VMEM((number, number), F32),),
    )
    return (preconditioned, turned.T, gram_matrix, new_block)


def solution(mesh):
    both = ("group", "member")
    placed = (
        P(both, None, None, None),
        P(both, None),
        P(both, None, None),
        P(both, None),
        P(both, None, None),
        P(both, None, None),
        P(both),
        P(both, None, None),
        P(None, "group"),
        P(both, None, None),
    )
    return jax.shard_map(
        local,
        mesh=mesh,
        in_specs=placed,
        out_specs=(P(both, None, None), P(), P(), P(both, None, None)),
        check_vma=False,
    )
```

```python
import functools

import jax
import jax.numpy as jnp
from jax import lax
from jax.experimental import pallas as pl
from jax.experimental.pallas import tpu as pltpu
from jax.sharding import PartitionSpec as P

AXES = ("group", "member")
F32 = jnp.float32
BF16 = jnp.bfloat16
HIGH = lax.Precision.HIGHEST


def dot(left, right, contract=(1, 0), precision=None):
    return lax.dot_general(
        left,
        right,
        (((contract[0],), (contract[1],)), ((), ())),
        precision=precision,
        preferred_element_type=F32,
    )


def place():
    group, member = lax.axis_index("group"), lax.axis_index("member")
    return group, member, lax.axis_size("group"), lax.axis_size("member")


def fill_halo(send_ref, tiles, choice_ref):
    group, _, _, members = place()
    slots = choice_ref.shape[0] // members
    for j, tile in enumerate(tiles):
        narrow = tile.astype(BF16)
        send_ref[:, j] = jnp.broadcast_to(narrow[None], (send_ref.shape[0], *tile.shape))
    for slot in range(slots):
        for peer in range(members):
            value = pick(choice_ref[slot * members + peer], tiles)
            send_ref[group * members + peer, slot] = value.astype(BF16)


def pick(which, tiles):
    value = jnp.zeros_like(tiles[0])
    for j, tile in enumerate(tiles):
        value = jnp.where(which == j, tile, value)
    return value


def gather_rows(ext_ref, tiles, got_ref, rim_ref, select_ref, ghosts):
    group, member, groups, members = place()
    count, (vectors, width) = len(tiles), tiles[0].shape
    rims = rim_ref.shape[0] // 2
    extended = ext_ref.shape[0]
    narrow = [None] * extended
    for j, tile in enumerate(tiles):
        ext_ref[j] = tile
    for slot in range(ghosts):
        for peer in range(members):
            ext_ref[count + peer * ghosts + slot] = got_ref[group * members + peer, slot].astype(F32)
    base = count + members * ghosts
    for side in range(2):
        other = jnp.clip(group - 1 + 2 * side, 0, groups - 1) * members + member
        found = [got_ref[other, j].astype(F32) for j in range(count)]
        for slot in range(rims):
            at = side * rims + slot
            ext_ref[base + at] = pick(rim_ref[at], found)
    extended_rows = ext_ref[...].reshape(extended * vectors, width).astype(BF16)
    return dot(select_ref[...], extended_rows).astype(BF16)


def apply_rows(picked, tiles, off_ref, diag_ref):
    count, (vectors, width) = len(tiles), tiles[0].shape
    number = off_ref.shape[1]
    results = []
    for t in range(count):
        rows = [picked[(t * number + k) * vectors : (t * number + k + 1) * vectors] for k in range(number)]
        left = jnp.concatenate(rows, axis=1)
        right = off_ref[t].reshape(number * width, width)
        results.append(dot(tiles[t].astype(BF16), diag_ref[t]) + dot(left, right))
    return results


def kernel_start(
    off_hbm, cols_hbm, member_send_hbm, group_send_hbm, diag_hbm, smoother_hbm, agg_hbm, prolong_hbm, basis_hbm,
    first_ref, send_ref, choice_ref, select_ref, mine_ref, off_ref, diag_ref, smoother_ref, prolong_ref, basis_ref,
    cols_ref, member_send_ref, group_send_ref, agg_ref, sems,
):
    count, vectors, width = first_ref.shape
    pairs = (
        (basis_hbm, basis_ref),
        (smoother_hbm, smoother_ref),
        (member_send_hbm, member_send_ref),
        (group_send_hbm, group_send_ref),
        (cols_hbm, cols_ref),
        (agg_hbm, agg_ref),
        (off_hbm, off_ref),
        (diag_hbm, diag_ref),
        (prolong_hbm, prolong_ref),
    )
    copies = [pltpu.make_async_copy(a, b, sems.at[i]) for i, (a, b) in enumerate(pairs)]
    for copy in copies:
        copy.start()
    for copy in copies[:6]:
        copy.wait()
    before = basis_ref.shape[1] - vectors
    tiles = []
    for t in range(count):
        value = dot(basis_ref[t, before:, :], smoother_ref[t]).astype(BF16)
        first_ref[t] = value
        tiles.append(value.astype(F32))
    for at in range(member_send_ref.shape[1]):
        choice_ref[at] = jnp.full((vectors, width), member_send_ref[0, at].astype(F32))
    fill_halo(send_ref, tiles, choice_ref)
    rows = lax.broadcasted_iota(jnp.int32, (vectors, width), 0)
    table = jnp.zeros((vectors, width), F32)
    for slot in range(group_send_ref.shape[1]):
        table = jnp.where(rows == slot, group_send_ref[0, slot].astype(F32), table)
    send_ref[:, send_ref.shape[1] - 1] = jnp.broadcast_to(
        table.astype(BF16)[None], (send_ref.shape[0], vectors, width)
    )
    number = off_ref.shape[1]
    columns = select_ref.shape[1]
    ahead = lax.broadcasted_iota(jnp.int32, (vectors, columns), 1) - lax.broadcasted_iota(
        jnp.int32, (vectors, columns), 0
    )
    for t in range(count):
        blocks = [jnp.where(ahead == cols_ref[t, k] * vectors, 1.0, 0.0) for k in range(number)]
        select_ref[t * number * vectors : (t + 1) * number * vectors, :] = jnp.concatenate(blocks, 0).astype(BF16)
        mine_ref[t] = jnp.full((vectors, width), agg_ref[t].astype(F32))
    for copy in copies[6:]:
        copy.wait()


def kernel_restrict(
    ghosts, first_ref, got_ref, select_ref, mine_ref, off_ref, diag_ref, prolong_ref, basis_ref,
    send_ref, rim_ref, ext_ref,
):
    group, member, groups, members = place()
    count, vectors, width = first_ref.shape
    before = basis_ref.shape[1] - vectors
    coarse = send_ref.shape[1]
    rims = rim_ref.shape[0] // 2
    for side in range(2):
        other = group - 1 + 2 * side
        inside = jnp.logical_and(other >= 0, other < groups)
        source = jnp.clip(other, 0, groups - 1) * members + member
        table = got_ref[source, got_ref.shape[1] - 1].astype(F32)
        table = jnp.where(inside, table, -1.0)
        for slot in range(rims):
            rim_ref[side * rims + slot] = jnp.broadcast_to(table[slot : slot + 1, :], (vectors, width))
    tiles = [first_ref[t].astype(F32) for t in range(count)]
    picked = gather_rows(ext_ref, tiles, got_ref, rim_ref, select_ref, ghosts)
    products = apply_rows(picked, tiles, off_ref, diag_ref)
    parts = [jnp.zeros((vectors, width), F32) for _ in range(coarse)]
    for t in range(count):
        right = basis_ref[t, before:, :].astype(F32)
        piece = dot((right - products[t]).astype(BF16), prolong_ref[t], (1, 1))
        for a in range(coarse):
            parts[a] = parts[a] + jnp.where(mine_ref[t] == a, piece, 0.0)
    for a in range(coarse):
        send_ref[:, a] = jnp.broadcast_to(parts[a].astype(BF16)[None], (send_ref.shape[0], vectors, width))


def kernel_coarse(got_ref, inverse_ref, first_ref, choice_ref, mine_ref, prolong_ref, second_ref, send_ref):
    _, _, groups, members = place()
    count, vectors, width = first_ref.shape
    coarse = got_ref.shape[1]
    sums = []
    for g in range(groups):
        for a in range(coarse):
            part = got_ref[g * members, a].astype(F32)
            for m in range(1, members):
                part = part + got_ref[g * members + m, a].astype(F32)
            sums.append(part.astype(BF16))
    total = dot(jnp.concatenate(sums, axis=1), inverse_ref[...])
    fixes = [total[:, a * width : (a + 1) * width] for a in range(coarse)]
    tiles = []
    for t in range(count):
        step = dot(pick(mine_ref[t], fixes).astype(BF16), prolong_ref[t])
        value = (first_ref[t].astype(F32) + step).astype(BF16)
        second_ref[t] = value
        tiles.append(value.astype(F32))
    fill_halo(send_ref, tiles, choice_ref)


def kernel_smooth(
    ghosts, second_ref, got_ref, rim_ref, select_ref, choice_ref, off_ref, diag_ref, smoother_ref, basis_ref,
    result_ref, send_ref, ext_ref,
):
    count, vectors, _ = second_ref.shape
    before = basis_ref.shape[1] - vectors
    tiles = [second_ref[t].astype(F32) for t in range(count)]
    picked = gather_rows(ext_ref, tiles, got_ref, rim_ref, select_ref, ghosts)
    products = apply_rows(picked, tiles, off_ref, diag_ref)
    results = []
    for t in range(count):
        right = basis_ref[t, before:, :].astype(F32)
        step = dot((right - products[t]).astype(BF16), smoother_ref[t])
        value = (tiles[t] + step).astype(BF16)
        result_ref[t] = value
        results.append(value.astype(F32))
    fill_halo(send_ref, results, choice_ref)


def pack_offsets(blocks):
    starts = []
    at = blocks + 1
    for i in range(blocks):
        starts.append(at)
        at += blocks - i
    return starts


def kernel_products(
    ghosts, values_ref, got_ref, rim_ref, select_ref, off_ref, diag_ref, basis_ref,
    applied_ref, send_ref, values_hbm, ext_ref, sem,
):
    out = pltpu.make_async_copy(values_ref, values_hbm, sem)
    out.start()
    count, vectors, width = values_ref.shape
    number = basis_ref.shape[1]
    blocks = number // vectors
    lanes = lax.broadcasted_iota(jnp.int32, (vectors, width), 1)
    wides = []
    packed = [jnp.zeros((vectors, width), F32) for _ in range(blocks)]
    for t in range(count):
        basis = basis_ref[t]
        wide = jnp.concatenate([basis, jnp.zeros((width - number, width), BF16)], axis=0)
        wides.append(wide)
        whole = dot(basis, wide, (1, 1))
        for i in range(blocks):
            packed[i] = packed[i] + whole[i * vectors : (i + 1) * vectors, :]
    total = jnp.zeros((vectors, width), F32)
    for i, start in enumerate(pack_offsets(blocks)):
        moved = pltpu.roll(packed[i], ((start - i) * vectors) % width, 1)
        inside = jnp.logical_and(lanes >= start * vectors, lanes < (start + blocks - i) * vectors)
        total = jnp.where(inside, moved, total)
    tiles = [values_ref[t].astype(F32) for t in range(count)]
    picked = gather_rows(ext_ref, tiles, got_ref, rim_ref, select_ref, ghosts)
    products = apply_rows(picked, tiles, off_ref, diag_ref)
    own = jnp.zeros((vectors, width), F32)
    for t in range(count):
        applied = products[t].astype(BF16)
        applied_ref[t] = applied
        total = total + dot(applied, wides[t], (1, 1))
        tall = jnp.concatenate([applied.astype(F32), jnp.zeros((width - vectors, width), F32)], axis=0)
        own = own + dot(applied, tall.astype(BF16), (1, 1))
    total = total + pltpu.roll(own, number, 1)
    send_ref[...] = jnp.broadcast_to(total[None], send_ref.shape)
    out.wait()


def kernel_finish(scale, got_ref, applied_ref, basis_ref, coefficients_ref, gram_ref, block_ref, half_ref):
    count, vectors, width = applied_ref.shape
    number = basis_ref.shape[1]
    blocks = number // vectors
    total = jnp.sum(got_ref[...], axis=0) * scale
    turned = total[:, :number]
    own = total[:, number : number + vectors]
    coefficients_ref[...] = turned
    lanes = lax.broadcasted_iota(jnp.int32, (vectors, width), 1)
    rows = lax.broadcasted_iota(jnp.int32, (vectors, width), 0)
    for i, start in enumerate(pack_offsets(blocks)):
        moved = pltpu.roll(total, (i - start) * vectors % width, 1)
        first, last = i * vectors, (i + 1) * vectors
        inside = jnp.logical_and(lanes >= first, lanes < last)
        unit = jnp.where(lanes == rows + first, 1.0, 0.0)
        beyond = jnp.logical_and(lanes >= last, lanes < number)
        value = jnp.where(inside, unit - 0.5 * moved, jnp.where(beyond, -moved, 0.0))
        half_ref[i * vectors : (i + 1) * vectors, :] = value[:, :number]
    half = half_ref[...]
    weighted = dot(turned, half, (1, 1), HIGH)
    gram = own - dot(turned, weighted, (1, 1), HIGH) - dot(weighted, turned, (1, 1), HIGH)
    gram_ref[...] = gram
    square = lax.broadcasted_iota(jnp.int32, (vectors, vectors), 1)
    level = lax.broadcasted_iota(jnp.int32, (vectors, vectors), 0)
    left = gram
    right = jnp.where(square == level, 1.0, 0.0)
    for j in range(vectors):
        pivot = jnp.sqrt(left[j : j + 1, j : j + 1])
        line_left = left[j : j + 1, :] / pivot
        line_right = right[j : j + 1, :] / pivot
        factor = left[:, j : j + 1] / pivot
        below = level > j
        left = jnp.where(below, left - factor * line_left, left)
        right = jnp.where(below, right - factor * line_right, jnp.where(level == j, line_right, right))
    for tile in range(count):
        basis = basis_ref[tile].astype(F32)
        remainder = applied_ref[tile].astype(F32) - dot(turned, basis, (1, 0), HIGH)
        block_ref[tile] = dot(right, remainder, (1, 0), HIGH)


def spread(blocks):
    return lax.all_to_all(blocks, AXES, split_axis=0, concat_axis=0, tiled=True)


def local(
    off_tiles,
    off_cols,
    member_send,
    group_send,
    diag_tiles,
    smoother,
    agg_map,
    prolong,
    coarse_inv,
    krylov_basis,
):
    members = lax.axis_size("member")
    devices = lax.axis_size("group") * members
    count, width, _ = diag_tiles.shape
    number = krylov_basis.shape[1]
    ghosts, rims = member_send.shape[2], group_send.shape[1]
    coarse = coarse_inv.shape[1] // width
    extended = count + members * ghosts + 2 * rims
    vectors = 8
    tile = (vectors, width)
    halo = max(count, ghosts)
    k = off_tiles.shape[1]
    smem, hbm = pltpu.SMEM, pl.BlockSpec(memory_space=pltpu.HBM)
    vmem = pl.BlockSpec(memory_space=pltpu.VMEM)
    shape = jax.ShapeDtypeStruct
    ext = pltpu.VMEM((extended, *tile), F32)
    own = shape((count, *tile), BF16)
    sent = shape((devices, halo, *tile), BF16)

    def call(body, outs, ins, scratch=(), in_spec=vmem, in_hbm=()):
        return pl.pallas_call(
            body,
            out_shape=tuple(outs) + tuple(in_hbm),
            in_specs=[in_spec] * len(ins),
            out_specs=(vmem,) * len(outs) + (hbm,) * len(in_hbm),
            scratch_shapes=scratch,
            compiler_params=pltpu.CompilerParams(vmem_limit_bytes=8 * 1024 * 1024),
        )(*ins)

    peers = jnp.transpose(member_send, (0, 2, 1)).reshape(1, ghosts * members)
    outs = call(
        kernel_start,
        (
            own,
            shape((devices, halo + 1, *tile), BF16),
            shape((ghosts * members, *tile), F32),
            shape((count * k * vectors, extended * vectors), BF16),
            shape((count, *tile), F32),
            *(shape(a.shape, a.dtype) for a in (off_tiles, diag_tiles, smoother, prolong, krylov_basis)),
        ),
        [
            pltpu.with_memory_space_constraint(a, pltpu.HBM)
            for a in (off_tiles, off_cols, peers, group_send, diag_tiles, smoother, agg_map, prolong, krylov_basis)
        ],
        (
            smem(off_cols.shape, jnp.int32),
            smem(peers.shape, jnp.int32),
            smem(group_send.shape, jnp.int32),
            smem(agg_map.shape, jnp.int32),
            pltpu.SemaphoreType.DMA((9,)),
        ),
        hbm,
    )
    first, send, choice, select, mine, off, diag, smooth, prolonged, basis = outs
    send, rim = call(
        functools.partial(kernel_restrict, ghosts),
        (shape((devices, coarse, *tile), BF16), shape((2 * rims, *tile), F32)),
        (first, spread(send), select, mine, off, diag, prolonged, basis),
        (ext,),
    )
    second, send = call(
        kernel_coarse, (own, sent), (spread(send), coarse_inv, first, choice, mine, prolonged)
    )
    result, send = call(
        functools.partial(kernel_smooth, ghosts),
        (own, sent),
        (second, spread(send), rim, select, choice, off, diag, smooth, basis),
        (ext,),
    )
    applied, send, preconditioned = call(
        functools.partial(kernel_products, ghosts),
        (own, shape((devices, *tile), F32)),
        (result, spread(send), rim, select, off, diag, basis),
        (ext, pltpu.SemaphoreType.DMA),
        in_hbm=(own,),
    )
    turned, gram_matrix, new_block = call(
        functools.partial(kernel_finish, 1.0 / (count * width * devices)),
        (shape((vectors, number), F32), shape((vectors, vectors), F32), shape((count, *tile), F32)),
        (spread(send), applied, basis),
        (pltpu.VMEM((number, number), F32),),
    )
    return (preconditioned, turned.T, gram_matrix, new_block)


def solution(mesh):
    both = ("group", "member")
    placed = (
        P(both, None, None, None),
        P(both, None),
        P(both, None, None),
        P(both, None),
        P(both, None, None),
        P(both, None, None),
        P(both),
        P(both, None, None),
        P(None, "group"),
        P(both, None, None),
    )
    return jax.shard_map(
        local,
        mesh=mesh,
        in_specs=placed,
        out_specs=(P(both, None, None), P(), P(), P(both, None, None)),
        check_vma=False,
    )
```

```python
import functools

import jax
import jax.numpy as jnp
from jax import lax
from jax.experimental import pallas as pl
from jax.experimental.pallas import tpu as pltpu
from jax.sharding import PartitionSpec as P


AXES = ("group", "member")
F32 = jnp.float32
BF16 = jnp.bfloat16
HIGH = lax.Precision.HIGHEST


def dot(left, right, contract=(1, 0), precision=None):
    return lax.dot_general(
        left,
        right,
        (((contract[0],), (contract[1],)), ((), ())),
        precision=precision,
        preferred_element_type=F32,
    )


def place():
    group, member = lax.axis_index("group"), lax.axis_index("member")
    return group, member, lax.axis_size("group"), lax.axis_size("member")


def fill_halo(send_ref, tiles, choice_ref):
    group, _, _, members = place()
    slots = choice_ref.shape[0] // members
    for j, tile in enumerate(tiles):
        narrow = tile.astype(BF16)
        send_ref[:, j] = jnp.broadcast_to(narrow[None], (send_ref.shape[0], *tile.shape))
    for slot in range(slots):
        for peer in range(members):
            value = pick(choice_ref[slot * members + peer], tiles)
            send_ref[group * members + peer, slot] = value.astype(BF16)


def pick(which, tiles):
    value = jnp.zeros_like(tiles[0])
    for j, tile in enumerate(tiles):
        value = jnp.where(which == j, tile, value)
    return value


def select_rows(ext_ref, tiles, select_ref):
    vectors, width = tiles[0].shape
    for j, tile in enumerate(tiles):
        ext_ref[j] = tile
    rows = ext_ref[...].reshape(ext_ref.shape[0] * vectors, width).astype(BF16)
    return dot(select_ref[...], rows).astype(BF16)


def place_rims(ext_ref, base, side, found, rim_ref):
    rims = rim_ref.shape[0] // 2
    for slot in range(rims):
        at = side * rims + slot
        ext_ref[base + at] = pick(rim_ref[at], found)


def sides():
    group, _, groups, _ = place()
    odd = lax.rem(group, 2)
    result = []
    for side in (1 - odd, odd):
        other = group - 1 + 2 * side
        result.append((side, jnp.logical_and(other >= 0, other < groups)))
    return result


def tail_of(ref, count, vectors):
    tail = ref[...].astype(F32)
    parts = [tail[i * vectors : (i + 1) * vectors] for i in range(2 * count + 1)]
    return parts[:count], parts[count], parts[count + 1 :]


def apply_rows(picked, tiles, off_ref, diag_ref):
    count, (vectors, width) = len(tiles), tiles[0].shape
    number = off_ref.shape[1]
    results = []
    for t in range(count):
        rows = [picked[(t * number + k) * vectors : (t * number + k + 1) * vectors] for k in range(number)]
        left = jnp.concatenate(rows, axis=1)
        right = off_ref[t].reshape(number * width, width)
        results.append(dot(tiles[t].astype(BF16), diag_ref[t]) + dot(left, right))
    return results


def kernel_start(
    smoother_hbm, prolong_hbm, basis_hbm, member_send_hbm, agg_hbm,
    first_ref, parcel_ref, choice_ref, mine_ref, smoother_ref, prolong_ref, basis_ref,
    member_send_ref, agg_ref, sems,
):
    count, vectors, width = first_ref.shape
    members, ghosts = parcel_ref.shape[:2]
    pairs = (
        (basis_hbm, basis_ref),
        (smoother_hbm, smoother_ref),
        (member_send_hbm, member_send_ref),
        (agg_hbm, agg_ref),
        (prolong_hbm, prolong_ref),
    )
    copies = [pltpu.make_async_copy(a, b, sems.at[i]) for i, (a, b) in enumerate(pairs)]
    for copy in copies:
        copy.start()
    for copy in copies:
        copy.wait()
    before = basis_ref.shape[1] - vectors
    tiles = []
    for t in range(count):
        value = dot(basis_ref[t, before:, :], smoother_ref[t]).astype(BF16)
        first_ref[t] = value
        tiles.append(value.astype(F32))
        mine_ref[t] = jnp.full((vectors, width), agg_ref[t].astype(F32))
    for slot in range(ghosts):
        for peer in range(members):
            number = member_send_ref[0, slot * members + peer]
            choice = jnp.full((vectors, width), number.astype(F32))
            choice_ref[slot * members + peer] = choice
            own = jnp.full((vectors, width), agg_ref[number].astype(F32))
            parcel_ref[peer, slot, :width] = prolong_ref[number]
            parcel_ref[peer, slot, width:] = jnp.concatenate([pick(choice, tiles), own], axis=0).astype(BF16)


def kernel_stage(
    off_hbm, diag_hbm, inverse_hbm, prolong_hbm, cols_hbm, group_send_hbm, first_ref, mine_ref,
    swap_ref, head_ref, select_ref, off_ref, diag_ref,
    cols_ref, group_send_ref, sems,
):
    count, vectors, width = first_ref.shape
    long, columns = inverse_hbm.shape
    coarse = columns // width
    pairs = [(cols_hbm, cols_ref), (group_send_hbm, group_send_ref)]
    for a in range(coarse):
        pairs.append((inverse_hbm.at[:, a * width : (a + 1) * width], swap_ref.at[a * long : (a + 1) * long, :]))
    at = coarse * long
    for t in range(count):
        pairs.append((prolong_hbm.at[t], swap_ref.at[at + t * width : at + (t + 1) * width, :]))
    pairs += [(off_hbm, off_ref), (diag_hbm, diag_ref)]
    copies = [pltpu.make_async_copy(a, b, sems.at[i]) for i, (a, b) in enumerate(pairs)]
    for copy in copies:
        copy.start()
    for copy in copies[:2]:
        copy.wait()
    rows = lax.broadcasted_iota(jnp.int32, (vectors, width), 0)
    table = jnp.zeros((vectors, width), F32)
    for slot in range(group_send_ref.shape[1]):
        table = jnp.where(rows == slot, group_send_ref[0, slot].astype(F32), table)
    tail = [first_ref[t].astype(F32) for t in range(count)] + [table] + [mine_ref[t] for t in range(count)]
    head_ref[...] = jnp.concatenate(tail + [jnp.zeros_like(table)], axis=0).astype(BF16)
    number = off_ref.shape[1]
    wide = select_ref.shape[1]
    ahead = lax.broadcasted_iota(jnp.int32, (vectors, wide), 1) - lax.broadcasted_iota(
        jnp.int32, (vectors, wide), 0
    )
    for t in range(count):
        blocks = [jnp.where(ahead == cols_ref[t, k] * vectors, 1.0, 0.0) for k in range(number)]
        select_ref[t * number * vectors : (t + 1) * number * vectors, :] = jnp.concatenate(blocks, 0).astype(BF16)
    for copy in copies[2:]:
        copy.wait()


def kernel_restrict(
    first_ref, parcel_ref, even_ref, odd_ref, select_ref, mine_ref, off_ref, diag_ref, prolong_ref, basis_ref,
    send_ref, rim_ref, ext_ref,
):
    count, vectors, width = first_ref.shape
    members, ghosts = parcel_ref.shape[:2]
    before = basis_ref.shape[1] - vectors
    coarse = send_ref.shape[1]
    rims = rim_ref.shape[0] // 2
    base = count + members * ghosts
    for ref, (side, exists) in zip((even_ref, odd_ref), sides(), strict=True):
        found, table, _ = tail_of(ref, count, vectors)
        table = jnp.where(exists, table, -1.0)
        for slot in range(rims):
            rim_ref[side * rims + slot] = jnp.broadcast_to(table[slot : slot + 1, :], (vectors, width))
        place_rims(ext_ref, base, side, found, rim_ref)
    tiles = [first_ref[t].astype(F32) for t in range(count)]
    arrived = [
        parcel_ref[peer, slot, width:].astype(F32)[:vectors] for peer in range(members) for slot in range(ghosts)
    ]
    picked = select_rows(ext_ref, tiles + arrived, select_ref)
    products = apply_rows(picked, tiles, off_ref, diag_ref)
    parts = [jnp.zeros((vectors, width), F32) for _ in range(coarse)]
    for t in range(count):
        right = basis_ref[t, before:, :].astype(F32)
        piece = dot((right - products[t]).astype(BF16), prolong_ref[t], (1, 1))
        for a in range(coarse):
            parts[a] = parts[a] + jnp.where(mine_ref[t] == a, piece, 0.0)
    for a in range(coarse):
        send_ref[:, a] = jnp.broadcast_to(parts[a].astype(BF16)[None], (send_ref.shape[0], vectors, width))


def corrected(first, which, fixes, prolong):
    return (first + dot(pick(which, fixes).astype(BF16), prolong)).astype(BF16).astype(F32)


def fixes_of(sums, ref, coarse):
    long = sums.shape[1]
    return [dot(sums, ref[a * long : (a + 1) * long, :]) for a in range(coarse)]


def kernel_sums(
    got_ref, first_ref, parcel_ref, swap_ref, mine_ref, prolong_ref,
    sums_ref, moved_ref,
):
    _, _, groups, members = place()
    count, _, width = first_ref.shape
    ghosts = parcel_ref.shape[1]
    coarse = got_ref.shape[1]
    sums = []
    for g in range(groups):
        for a in range(coarse):
            part = got_ref[g * members, a].astype(F32)
            for m in range(1, members):
                part = part + got_ref[g * members + m, a].astype(F32)
            sums.append(part.astype(BF16))
    sums = jnp.concatenate(sums, axis=1)
    sums_ref[...] = sums
    fixes = fixes_of(sums, swap_ref, coarse)
    for t in range(count):
        moved_ref[t] = corrected(first_ref[t].astype(F32), mine_ref[t], fixes, prolong_ref[t])
    for peer in range(members):
        for slot in range(ghosts):
            end = parcel_ref[peer, slot, width:].astype(F32)
            vectors = end.shape[0] // 2
            value = corrected(end[:vectors], end[vectors:], fixes, parcel_ref[peer, slot, :width])
            moved_ref[count + peer * ghosts + slot] = value


def kernel_cycle(
    sums_ref, moved_ref, even_ref, odd_ref, even_head_ref, odd_head_ref, rim_ref, select_ref, choice_ref,
    off_ref, diag_ref, smoother_ref, basis_ref,
    result_ref, send_ref, ext_ref,
):
    count, vectors, width = result_ref.shape
    before = basis_ref.shape[1] - vectors
    sums = sums_ref[...]
    at = even_ref.shape[0] - count * width
    coarse = at // sums.shape[1]
    base = moved_ref.shape[0]
    swapped = ((even_ref, even_head_ref), (odd_ref, odd_head_ref))
    for (ref, head_ref), (side, _) in zip(swapped, sides(), strict=True):
        fixes = fixes_of(sums, ref, coarse)
        found, _, theirs = tail_of(head_ref, count, vectors)
        found = [
            corrected(found[t], theirs[t], fixes, ref[at + t * width : at + (t + 1) * width, :])
            for t in range(count)
        ]
        place_rims(ext_ref, base, side, found, rim_ref)
    moved = [moved_ref[e] for e in range(base)]
    tiles = moved[:count]
    picked = select_rows(ext_ref, moved, select_ref)
    products = apply_rows(picked, tiles, off_ref, diag_ref)
    results = []
    for t in range(count):
        right = basis_ref[t, before:, :].astype(F32)
        step = dot((right - products[t]).astype(BF16), smoother_ref[t])
        value = (tiles[t] + step).astype(BF16)
        result_ref[t] = value
        results.append(value.astype(F32))
    fill_halo(send_ref, results, choice_ref)


def pack_offsets(blocks):
    starts = []
    at = blocks + 1
    for i in range(blocks):
        starts.append(at)
        at += blocks - i
    return starts


def kernel_products(
    ghosts, values_ref, got_ref, rim_ref, select_ref, off_ref, diag_ref, basis_ref,
    applied_ref, send_ref, values_hbm, ext_ref, sem,
):
    out = pltpu.make_async_copy(values_ref, values_hbm, sem)
    out.start()
    count, vectors, width = values_ref.shape
    number = basis_ref.shape[1]
    blocks = number // vectors
    lanes = lax.broadcasted_iota(jnp.int32, (vectors, width), 1)
    wides = []
    packed = [jnp.zeros((vectors, width), F32) for _ in range(blocks)]
    for t in range(count):
        basis = basis_ref[t]
        wide = jnp.concatenate([basis, jnp.zeros((width - number, width), BF16)], axis=0)
        wides.append(wide)
        whole = dot(basis, wide, (1, 1))
        for i in range(blocks):
            packed[i] = packed[i] + whole[i * vectors : (i + 1) * vectors, :]
    total = jnp.zeros((vectors, width), F32)
    for i, start in enumerate(pack_offsets(blocks)):
        moved = pltpu.roll(packed[i], ((start - i) * vectors) % width, 1)
        inside = jnp.logical_and(lanes >= start * vectors, lanes < (start + blocks - i) * vectors)
        total = jnp.where(inside, moved, total)
    tiles = [values_ref[t].astype(F32) for t in range(count)]
    group, member, groups, members = place()
    arrived = [
        got_ref[group * members + peer, slot].astype(F32) for peer in range(members) for slot in range(ghosts)
    ]
    for side in range(2):
        other = jnp.clip(group - 1 + 2 * side, 0, groups - 1) * members + member
        found = [got_ref[other, j].astype(F32) for j in range(count)]
        place_rims(ext_ref, count + len(arrived), side, found, rim_ref)
    picked = select_rows(ext_ref, tiles + arrived, select_ref)
    products = apply_rows(picked, tiles, off_ref, diag_ref)
    own = jnp.zeros((vectors, width), F32)
    for t in range(count):
        applied = products[t].astype(BF16)
        applied_ref[t] = applied
        total = total + dot(applied, wides[t], (1, 1))
        tall = jnp.concatenate([applied.astype(F32), jnp.zeros((width - vectors, width), F32)], axis=0)
        own = own + dot(applied, tall.astype(BF16), (1, 1))
    total = total + pltpu.roll(own, number, 1)
    send_ref[...] = jnp.broadcast_to(total[None], send_ref.shape)
    out.wait()


def kernel_finish(scale, got_ref, applied_ref, basis_ref, coefficients_ref, gram_ref, block_ref, half_ref):
    count, vectors, width = applied_ref.shape
    number = basis_ref.shape[1]
    blocks = number // vectors
    total = jnp.sum(got_ref[...], axis=0) * scale
    turned = total[:, :number]
    own = total[:, number : number + vectors]
    coefficients_ref[...] = turned
    lanes = lax.broadcasted_iota(jnp.int32, (vectors, width), 1)
    rows = lax.broadcasted_iota(jnp.int32, (vectors, width), 0)
    for i, start in enumerate(pack_offsets(blocks)):
        moved = pltpu.roll(total, (i - start) * vectors % width, 1)
        first, last = i * vectors, (i + 1) * vectors
        inside = jnp.logical_and(lanes >= first, lanes < last)
        unit = jnp.where(lanes == rows + first, 1.0, 0.0)
        beyond = jnp.logical_and(lanes >= last, lanes < number)
        value = jnp.where(inside, unit - 0.5 * moved, jnp.where(beyond, -moved, 0.0))
        half_ref[i * vectors : (i + 1) * vectors, :] = value[:, :number]
    half = half_ref[...]
    weighted = dot(turned, half, (1, 1), HIGH)
    gram = own - dot(turned, weighted, (1, 1), HIGH) - dot(weighted, turned, (1, 1), HIGH)
    gram_ref[...] = gram
    square = lax.broadcasted_iota(jnp.int32, (vectors, vectors), 1)
    level = lax.broadcasted_iota(jnp.int32, (vectors, vectors), 0)
    left = gram
    right = jnp.where(square == level, 1.0, 0.0)
    for j in range(vectors):
        pivot = jnp.sqrt(left[j : j + 1, j : j + 1])
        line_left = left[j : j + 1, :] / pivot
        line_right = right[j : j + 1, :] / pivot
        factor = left[:, j : j + 1] / pivot
        below = level > j
        left = jnp.where(below, left - factor * line_left, left)
        right = jnp.where(below, right - factor * line_right, jnp.where(level == j, line_right, right))
    for tile in range(count):
        basis = basis_ref[tile].astype(F32)
        remainder = applied_ref[tile].astype(F32) - dot(turned, basis, (1, 0), HIGH)
        block_ref[tile] = dot(right, remainder, (1, 0), HIGH)


def spread(blocks):
    return lax.all_to_all(blocks, AXES, split_axis=0, concat_axis=0, tiled=True)


def local(
    off_tiles,
    off_cols,
    member_send,
    group_send,
    diag_tiles,
    smoother,
    agg_map,
    prolong,
    coarse_inv,
    krylov_basis,
):
    members = lax.axis_size("member")
    devices = lax.axis_size("group") * members
    count, width, _ = diag_tiles.shape
    number = krylov_basis.shape[1]
    ghosts, rims = member_send.shape[2], group_send.shape[1]
    coarse = coarse_inv.shape[1] // width
    extended = count + members * ghosts + 2 * rims
    vectors = 8
    tile = (vectors, width)
    halo = max(count, ghosts)
    k = off_tiles.shape[1]
    smem, hbm = pltpu.SMEM, pl.BlockSpec(memory_space=pltpu.HBM)
    vmem = pl.BlockSpec(memory_space=pltpu.VMEM)
    shape = jax.ShapeDtypeStruct
    ext = pltpu.VMEM((extended, *tile), F32)
    own = shape((count, *tile), BF16)
    sent = shape((devices, halo, *tile), BF16)

    def call(body, outs, ins, scratch=(), in_specs=None, in_hbm=()):
        return pl.pallas_call(
            body,
            out_shape=tuple(outs) + tuple(in_hbm),
            in_specs=in_specs or [vmem] * len(ins),
            out_specs=(vmem,) * len(outs) + (hbm,) * len(in_hbm),
            scratch_shapes=scratch,
            compiler_params=pltpu.CompilerParams(vmem_limit_bytes=8 * 1024 * 1024),
        )(*ins)

    def stay(*arrays):
        return [pltpu.with_memory_space_constraint(a, pltpu.HBM) for a in arrays]

    groups = devices // members
    peers = jnp.transpose(member_send, (0, 2, 1)).reshape(1, ghosts * members)
    first, parcel, choice, mine, smooth, prolonged, basis = call(
        kernel_start,
        (
            own,
            shape((members, ghosts, width + 2 * vectors, width), BF16),
            shape((ghosts * members, *tile), F32),
            shape((count, *tile), F32),
            *(shape(a.shape, a.dtype) for a in (smoother, prolong, krylov_basis)),
        ),
        stay(smoother, prolong, krylov_basis, peers, agg_map),
        (smem(peers.shape, jnp.int32), smem(agg_map.shape, jnp.int32), pltpu.SemaphoreType.DMA((5,))),
        [hbm] * 5,
    )
    rows = coarse * coarse_inv.shape[0] + count * width
    swap, head, select, off, diag = call(
        kernel_stage,
        (
            shape((rows, width), BF16),
            shape((vectors * (2 * count + 2), width), BF16),
            shape((count * k * vectors, extended * vectors), BF16),
            *(shape(a.shape, a.dtype) for a in (off_tiles, diag_tiles)),
        ),
        [*stay(off_tiles, diag_tiles, coarse_inv, prolong, off_cols, group_send), first, mine],
        (
            smem(off_cols.shape, jnp.int32),
            smem(group_send.shape, jnp.int32),
            pltpu.SemaphoreType.DMA((4 + coarse + count,)),
        ),
        [hbm] * 6 + [vmem] * 2,
    )
    parcel = lax.all_to_all(parcel, "member", split_axis=0, concat_axis=0, tiled=True)
    pairs = [
        [(i + a, i + 1 - a) for i in range(start, groups - 1, 2) for a in (0, 1)] for start in (0, 1)
    ]
    even_head, odd_head = (lax.ppermute(head, "group", p) for p in pairs)
    even, odd = (lax.ppermute(swap, "group", p) for p in pairs)
    send, rim = call(
        kernel_restrict,
        (shape((devices, coarse, *tile), BF16), shape((2 * rims, *tile), F32)),
        (first, parcel, even_head, odd_head, select, mine, off, diag, prolonged, basis),
        (ext,),
    )
    sums, moved = call(
        kernel_sums,
        (shape((vectors, coarse_inv.shape[0]), BF16), shape((count + ghosts * members, *tile), F32)),
        (spread(send), first, parcel, swap, mine, prolonged),
    )
    result, send = call(
        kernel_cycle,
        (own, sent),
        (
            sums, moved, even, odd, even_head, odd_head, rim, select, choice,
            off, diag, smooth, basis,
        ),
        (ext,),
    )
    applied, send, preconditioned = call(
        functools.partial(kernel_products, ghosts),
        (own, shape((devices, *tile), F32)),
        (result, spread(send), rim, select, off, diag, basis),
        (ext, pltpu.SemaphoreType.DMA),
        in_hbm=(own,),
    )
    turned, gram_matrix, new_block = call(
        functools.partial(kernel_finish, 1.0 / (count * width * devices)),
        (shape((vectors, number), F32), shape((vectors, vectors), F32), shape((count, *tile), F32)),
        (spread(send), applied, basis),
        (pltpu.VMEM((number, number), F32),),
    )
    return (preconditioned, turned.T, gram_matrix, new_block)


def solution(mesh):
    both = ("group", "member")
    placed = (
        P(both, None, None, None),
        P(both, None),
        P(both, None, None),
        P(both, None),
        P(both, None, None),
        P(both, None, None),
        P(both),
        P(both, None, None),
        P(None, "group"),
        P(both, None, None),
    )

    return jax.shard_map(
        local,
        mesh=mesh,
        in_specs=placed,
        out_specs=(P(both, None, None), P(), P(), P(both, None, None)),
        check_vma=False,
    )
```
